32 devices in a mesh: gx: 4 (over x, core), gy: 4 (over z), gz: 2 (over y).
Axes of the slice: x: 2, y: 2, z: 4, core: 2. Of those that a mesh axis runs over, the one named last changes fastest.
Arguments:
- conserved_state: float32 [6, 16, 32, 240], P(None, 'gx', 'gy', 'gz'), as said below
Outputs:
- updated_state: float32 [6, 16, 32, 240], P(None, 'gx', 'gy', 'gz')
- next_timestep: float32 [], replicated
Inputs may be any that keep to these rules, and one draw needn't show every extreme that they name: `conserved_state`: component 0 is density within 0.5 to 3, components 1 to 3 are density times velocities each within -1 to 1, component 4 is total energy with pressure within 0.5 to 6, component 5 is density times a tracer fraction within 0 to 1.
All inputs are finite; a program needn't handle non-finite values.
Results may differ from the reference program's by a relative error of at most 0.0003.
Values sent between devices are 32-bit elements; how exact they have to be, the bound alone decides.
A program may use at most 64 MiB of HBM per device.

```python
import math
import jax
import jax.numpy as jnp
from jax import lax

CX = 4
GHOST = 4
NX = 16
NY = 32
NZ = 240


def draw_conserved_state(key, part):
    subkeys = jax.random.split(key, 6)
    grid_shape = (NX, NY, NZ)
    across = lax.broadcasted_iota(jnp.float32, grid_shape, 0) / NX
    density = jnp.exp(jax.random.uniform(subkeys[0], grid_shape, jnp.float32, math.log(0.5), math.log(2.0)))
    pressure = jnp.exp(jax.random.uniform(subkeys[1], grid_shape, jnp.float32, math.log(0.5), math.log(2.0)))
    tracer = jax.random.uniform(subkeys[5], grid_shape, jnp.float32, 0.0, 1.0)
    pressure = pressure * (1.0 + 2.0 * across)
    velocity = [jnp.clip(0.25 * jax.random.normal(subkeys[component], grid_shape, jnp.float32), -1.0, 1.0) for component in (2, 3, 4)]
    kinetic = 0.5 * density * (velocity[0] * velocity[0] + velocity[1] * velocity[1] + velocity[2] * velocity[2])
    energy = pressure / (5.0 / 3.0 - 1.0) + kinetic
    return jnp.stack([density, density * velocity[0], density * velocity[1], density * velocity[2], energy, density * tracer]).astype(jnp.float32)


def setup_inputs(seed: int = 0) -> dict:
    keys = jax.random.split(jax.random.key(seed), 2)
    return {
        "conserved_state": draw_conserved_state(jax.random.fold_in(keys[1], 71), 0),
    }


adiabatic = 5.0 / 3.0
courant = 0.3

def shifted(values, sweep_axis, offset):
    return jnp.roll(values, -offset, axis=sweep_axis)

def primitive_of(conserved_list):
    density = conserved_list[0]
    inverse = 1.0 / density
    velocity = [conserved_list[component] * inverse for component in (1, 2, 3)]
    kinetic = 0.5 * (conserved_list[1] * velocity[0] + conserved_list[2] * velocity[1] + conserved_list[3] * velocity[2])
    pressure = (adiabatic - 1.0) * (conserved_list[4] - kinetic)
    return [density, velocity[0], velocity[1], velocity[2], pressure, conserved_list[5] * inverse]

def conserved_of(primitive):
    density = primitive[0]
    momenta = [density * primitive[component] for component in (1, 2, 3)]
    kinetic = 0.5 * (momenta[0] * primitive[1] + momenta[1] * primitive[2] + momenta[2] * primitive[3])
    energy = primitive[4] / (adiabatic - 1.0) + kinetic
    return [density, momenta[0], momenta[1], momenta[2], energy, density * primitive[5]]

def fastest_signal(conserved_list):
    primitive = primitive_of(conserved_list)
    sound = jnp.sqrt(adiabatic * primitive[4] / primitive[0])
    speeds = jnp.maximum(jnp.maximum(jnp.abs(primitive[1]), jnp.abs(primitive[2])), jnp.abs(primitive[3]))
    return jnp.max(speeds + sound)

def parabola(centre, sweep_axis):
    before_one = shifted(centre, sweep_axis, -1)
    before_two = shifted(centre, sweep_axis, -2)
    before_three = shifted(centre, sweep_axis, -3)
    after_one = shifted(centre, sweep_axis, 1)
    after_two = shifted(centre, sweep_axis, 2)
    edge = (37.0 * (before_one + centre) - 8.0 * (before_two + after_one) + (before_three + after_two)) / 60.0
    edge = jnp.clip(edge, jnp.minimum(before_one, centre), jnp.maximum(before_one, centre))
    lower = edge
    upper = shifted(edge, sweep_axis, 1)
    flatten = (upper - centre) * (centre - lower) <= 0.0
    spread = upper - lower
    skewed = spread * (centre - 0.5 * (lower + upper))
    limit = spread * spread / 6.0
    new_lower = jnp.where(flatten, centre, jnp.where(skewed > limit, 3.0 * centre - 2.0 * upper, lower))
    new_upper = jnp.where(flatten, centre, jnp.where(skewed < -limit, 3.0 * centre - 2.0 * lower, upper))
    return (new_lower, new_upper)

def traced_faces(primitive, sweep_axis, time_step):
    normal = 1 + sweep_axis
    edges = [parabola(item, sweep_axis) for item in primitive]
    slopes = [pair[1] - pair[0] for pair in edges]
    normal_vel = primitive[normal]
    density = primitive[0]
    rates = [-(normal_vel * slopes[0] + density * slopes[normal])]
    for component in (1, 2, 3):
        if component == normal:
            rates.append(-(normal_vel * slopes[normal] + slopes[4] / density))
        else:
            rates.append(-normal_vel * slopes[component])
    rates.append(-(adiabatic * primitive[4] * slopes[normal] + normal_vel * slopes[4]))
    rates.append(-normal_vel * slopes[5])
    lower_faces = [edges[component][0] + 0.5 * time_step * rates[component] for component in range(6)]
    upper_faces = [edges[component][1] + 0.5 * time_step * rates[component] for component in range(6)]
    return (lower_faces, upper_faces)

def physical_flux(primitive, conserved_list, normal):
    normal_vel = primitive[normal]
    result = [item * normal_vel for item in conserved_list]
    result[normal] = result[normal] + primitive[4]
    result[4] = result[4] + primitive[4] * normal_vel
    return result

def star_state(primitive, conserved_list, outer_speed, middle_speed, normal):
    mass_rate = primitive[0] * (outer_speed - primitive[normal])
    factor = mass_rate / (outer_speed - middle_speed)
    result = [factor * primitive[component] for component in range(6)]
    result[0] = factor
    result[normal] = factor * middle_speed
    result[4] = factor * (conserved_list[4] / primitive[0] + (middle_speed - primitive[normal]) * (middle_speed + primitive[4] / mass_rate))
    return result

def hllc_flux(left, right, sweep_axis):
    normal = 1 + sweep_axis
    sound_left = jnp.sqrt(adiabatic * left[4] / left[0])
    sound_right = jnp.sqrt(adiabatic * right[4] / right[0])
    low_speed = jnp.minimum(left[normal] - sound_left, right[normal] - sound_right)
    high_speed = jnp.maximum(left[normal] + sound_left, right[normal] + sound_right)
    mass_left = left[0] * (low_speed - left[normal])
    mass_right = right[0] * (high_speed - right[normal])
    middle = (right[4] - left[4] + mass_left * left[normal] - mass_right * right[normal]) / (mass_left - mass_right)
    left_state = conserved_of(left)
    right_state = conserved_of(right)
    flux_left = physical_flux(left, left_state, normal)
    flux_right = physical_flux(right, right_state, normal)
    star_left = star_state(left, left_state, low_speed, middle, normal)
    star_right = star_state(right, right_state, high_speed, middle, normal)
    result = []
    for component in range(6):
        left_star_flux = flux_left[component] + low_speed * (star_left[component] - left_state[component])
        right_star_flux = flux_right[component] + high_speed * (star_right[component] - right_state[component])
        chosen = jnp.where(high_speed > 0.0, right_star_flux, flux_right[component])
        chosen = jnp.where(middle >= 0.0, left_star_flux, chosen)
        chosen = jnp.where(low_speed >= 0.0, flux_left[component], chosen)
        result.append(chosen)
    return result

def hydro_step(padded, time_step):
    conserved_list = [padded[component] for component in range(6)]
    primitive = primitive_of(conserved_list)
    faces = [traced_faces(primitive, sweep_axis, time_step) for sweep_axis in range(3)]
    predicted = []
    for sweep_axis in range(3):
        lower_faces, upper_faces = faces[sweep_axis]
        from_below = [shifted(item, sweep_axis, -1) for item in upper_faces]
        predicted.append(hllc_flux(from_below, lower_faces, sweep_axis))
    final_fluxes = []
    for sweep_axis in range(3):
        lower_faces, upper_faces = faces[sweep_axis]
        lower_state = conserved_of(lower_faces)
        upper_state = conserved_of(upper_faces)
        for other_axis in range(3):
            if other_axis != sweep_axis:
                for component in range(6):
                    flux_other = predicted[other_axis][component]
                    divergence = 0.5 * time_step * (shifted(flux_other, other_axis, 1) - flux_other)
                    lower_state[component] = lower_state[component] - divergence
                    upper_state[component] = upper_state[component] - divergence
        lower_prim = primitive_of(lower_state)
        upper_prim = primitive_of(upper_state)
        from_below = [shifted(item, sweep_axis, -1) for item in upper_prim]
        final_fluxes.append(hllc_flux(from_below, lower_prim, sweep_axis))
    updated = []
    for component in range(6):
        total = conserved_list[component]
        for sweep_axis in range(3):
            flux_here = final_fluxes[sweep_axis][component]
            total = total - time_step * (shifted(flux_here, sweep_axis, 1) - flux_here)
        updated.append(total[GHOST:-GHOST, GHOST:-GHOST, GHOST:-GHOST])
    return jnp.stack(updated)

def reference(conserved_state):
    slab_count = NX // CX
    indices = jnp.arange(slab_count).astype(jnp.int32)

    def slab_signal(slab_index):
        slab = lax.dynamic_slice_in_dim(conserved_state, slab_index * CX, CX, 1)
        return fastest_signal([slab[component] for component in range(6)])
    signal_now = jnp.max(lax.map(slab_signal, indices))
    time_step = courant / signal_now

    def slab_update(slab_index):
        plane_rows = (slab_index * CX - GHOST + jnp.arange(CX + 2 * GHOST).astype(jnp.int32)) % NX
        slab = jnp.take(conserved_state, plane_rows.astype(jnp.int32), axis=1)
        padded = jnp.pad(slab, ((0, 0), (0, 0), (GHOST, GHOST), (GHOST, GHOST)), mode='wrap')
        updated = hydro_step(padded, time_step)
        return (updated, fastest_signal([updated[component] for component in range(6)]))
    blocks, signals = lax.map(slab_update, indices)
    updated_state = jnp.transpose(blocks, (1, 0, 2, 3, 4)).reshape(6, NX, NY, NZ)
    next_timestep = courant / jnp.max(signals)
    return (updated_state, next_timestep)
```

```python
import functools

import jax
import jax.numpy as jnp
from jax import lax
from jax.experimental import pallas as pl
from jax.experimental.pallas import tpu as pltpu
from jax.sharding import PartitionSpec as P

GHOST = 4
ROWS = 8
LANES = 128
COMPS = 6

adiabatic = 5.0 / 3.0
courant = 0.3
MESH_ID = pl.DeviceIdType.MESH


def primitive_of(u):
    inverse = 1.0 / u[0]
    velocity = [u[component] * inverse for component in (1, 2, 3)]
    kinetic = 0.5 * (u[1] * velocity[0] + u[2] * velocity[1] + u[3] * velocity[2])
    pressure = (adiabatic - 1.0) * (u[4] - kinetic)
    return [u[0], velocity[0], velocity[1], velocity[2], pressure, u[5] * inverse]


def conserved_of(q):
    density = q[0]
    momenta = [density * q[component] for component in (1, 2, 3)]
    kinetic = 0.5 * (momenta[0] * q[1] + momenta[1] * q[2] + momenta[2] * q[3])
    energy = q[4] * (1.0 / (adiabatic - 1.0)) + kinetic
    return [density, momenta[0], momenta[1], momenta[2], energy, density * q[5]]


def signal_of(u):
    q = primitive_of(u)
    sound = jnp.sqrt(adiabatic * q[4] / q[0])
    return jnp.maximum(jnp.maximum(jnp.abs(q[1]), jnp.abs(q[2])), jnp.abs(q[3])) + sound


def edge_of(b3, b2, b1, c, a1, a2):
    edge = (37.0 * (b1 + c) - 8.0 * (b2 + a1) + (b3 + a2)) * (1.0 / 60.0)
    return jnp.minimum(jnp.maximum(edge, jnp.minimum(b1, c)), jnp.maximum(b1, c))


def limited(lower, upper, centre):
    flatten = (upper - centre) * (centre - lower) <= 0.0
    spread = upper - lower
    skewed = spread * (centre - 0.5 * (lower + upper))
    limit = spread * spread * (1.0 / 6.0)
    new_lower = jnp.where(skewed > limit, 3.0 * centre - 2.0 * upper, lower)
    new_upper = jnp.where(skewed < -limit, 3.0 * centre - 2.0 * lower, upper)
    return jnp.where(flatten, centre, new_lower), jnp.where(flatten, centre, new_upper)


def traced(q, edges, axis, half):
    normal = 1 + axis
    slopes = [pair[1] - pair[0] for pair in edges]
    n = q[normal] * half
    rates = []
    for component in range(COMPS):
        rate = n * slopes[component]
        if component == 0:
            rate = rate + (q[0] * half) * slopes[normal]
        elif component == normal:
            rate = rate + (half / q[0]) * slopes[4]
        elif component == 4:
            rate = rate + (adiabatic * half) * q[4] * slopes[normal]
        rates.append(rate)
    lower = [edges[component][0] - rates[component] for component in range(COMPS)]
    upper = [edges[component][1] - rates[component] for component in range(COMPS)]
    return lower, upper


def hllc(left, right, axis):
    normal = 1 + axis
    t1, t2 = [component for component in (1, 2, 3) if component != normal]
    ratio_l = left[4] / left[0]
    ratio_r = right[4] / right[0]
    sound_l = jnp.sqrt(adiabatic * ratio_l)
    sound_r = jnp.sqrt(adiabatic * ratio_r)
    n_l, n_r = left[normal], right[normal]
    low = jnp.minimum(n_l - sound_l, n_r - sound_r)
    high = jnp.maximum(n_l + sound_l, n_r + sound_r)
    mass_l = left[0] * (low - n_l)
    mass_r = right[0] * (high - n_r)
    middle = (right[4] - left[4] + mass_l * n_l - mass_r * n_r) / (mass_l - mass_r)
    on_left = middle >= 0.0
    pick = lambda a, b: jnp.where(on_left, a, b)
    r, n, p = pick(left[0], right[0]), pick(n_l, n_r), pick(left[4], right[4])
    v, w, tracer = pick(left[t1], right[t1]), pick(left[t2], right[t2]), pick(left[5], right[5])
    ratio, mass = pick(ratio_l, ratio_r), pick(mass_l, mass_r)
    outer = pick(low, high)
    speed = pick(jnp.minimum(low, 0.0), jnp.maximum(high, 0.0))
    factor = mass / (outer - middle)
    flux = r * n + speed * (factor - r)
    gain = speed * factor * (middle - n)
    energy = ratio * (1.0 / (adiabatic - 1.0)) + 0.5 * (n * n + v * v + w * w)
    result = [None] * COMPS
    result[0] = flux
    result[normal] = n * flux + p + gain
    result[t1] = v * flux
    result[t2] = w * flux
    result[4] = energy * flux + n * p + gain * (middle + p / mass)
    result[5] = tracer * flux
    return result


def rolled(x, offset, axis):
    return pltpu.roll(x, (-offset) % x.shape[axis], axis)


def kernel(sizes, u_hbm, out_ref, next_ref, own, rx, ysend, ry, y1send, zsend, rz, rxy, rxy1, u, q,
           face, pred, msend, mrecv, own_sem, send_sem, recv_sem, msend_sem, mrecv_sem):
    nx, ny, nz = sizes
    devices = nx * ny * nz
    comps, cx, cy, cz = own.shape
    slots = LANES // GHOST
    ix, iy, iz = lax.axis_index("gx"), lax.axis_index("gy"), lax.axis_index("gz")
    me = (ix * ny + iy) * nz + iz

    load = pltpu.make_async_copy(u_hbm, own, own_sem)
    load.start()

    def place(k):
        target = lax.rem(me + k, devices)
        return (lax.div(target, ny * nz), lax.rem(lax.div(target, nz), ny), lax.rem(target, nz))

    barrier = pltpu.get_barrier_semaphore()

    def greet(k, carry):
        pl.semaphore_signal(barrier, inc=1, device_id=place(k), device_id_type=MESH_ID)
        return carry

    lax.fori_loop(1, devices, greet, 0)
    load.wait()

    lane = lax.broadcasted_iota(jnp.int32, (ROWS, LANES), 1)
    row = lax.broadcasted_iota(jnp.int32, (ROWS, LANES), 0)
    upper_half = row < GHOST
    zero_tail = jnp.zeros((ROWS, LANES - cz), jnp.float32)

    def body(ref, c, x):
        return jnp.concatenate([ref[c, x], zero_tail], axis=1)

    tiles = [[body(own, c, x) for x in range(cx)] for c in range(COMPS)]
    best = None
    for x in range(cx):
        speeds = signal_of([tiles[c][x] for c in range(COMPS)])
        best = speeds if best is None else jnp.maximum(best, speeds)
    best = jnp.max(jnp.where(lane < cz, best, 0.0), axis=0, keepdims=True)
    msend[0] = best
    packs = [[None, None] for _ in range(zsend.shape[1])]
    for c in range(COMPS):
        for x in range(cx):
            slot = c * cx + x
            block, at = slot // slots, slot % slots * GHOST
            inside = (lane >= at) & (lane < at + GHOST)
            for side in range(2):
                start = 0 if side == 0 else cz - GHOST
                moved = pltpu.roll(tiles[c][x], (at - start) % LANES, 1)
                held = packs[block][side]
                packs[block][side] = moved if held is None else jnp.where(inside, moved, held)
    for block in range(zsend.shape[1]):
        for side in range(2):
            zsend[side, block] = packs[block][side]
    for x in range(cx):
        for pair in range(COMPS // 2):
            first, second = tiles[2 * pair][x], tiles[2 * pair + 1][x]
            swapped = pltpu.roll(second, GHOST, 0)
            ysend[0, x, pair] = jnp.where(upper_half, first, swapped)
            ysend[1, x, pair] = jnp.where(upper_half, swapped, first)
        for c in range(COMPS):
            y1send[0, x, c : c + 1] = tiles[c][x][0:1]
            y1send[1, x, c : c + 1] = tiles[c][x][ROWS - 1 : ROWS]

    pl.semaphore_wait(barrier, devices - 1)

    copies = []

    def send(src, dst, dx, dy, dz):
        number = len(copies)
        copy = pltpu.make_async_remote_copy(
            src_ref=src, dst_ref=dst, send_sem=send_sem.at[number], recv_sem=recv_sem.at[number],
            device_id=(lax.rem(ix + dx + nx, nx), lax.rem(iy + dy + ny, ny), lax.rem(iz + dz + nz, nz)),
            device_id_type=MESH_ID)
        copy.start()
        copies.append(copy)

    for dx in (-1, 1):
        send(own, rx.at[(1 - dx) // 2], dx, 0, 0)

    def share(turn):
        def one(k, carry):
            pltpu.make_async_remote_copy(
                src_ref=msend.at[turn], dst_ref=mrecv.at[turn, k - 1], send_sem=msend_sem.at[turn],
                recv_sem=mrecv_sem.at[turn], device_id=place(k), device_id_type=MESH_ID).start()
            return carry
        lax.fori_loop(1, devices, one, 0)

    def gather(turn):
        pltpu.make_async_copy(mrecv.at[turn], mrecv.at[turn], mrecv_sem.at[turn]).wait()
        pltpu.make_async_copy(mrecv.at[turn], mrecv.at[turn], msend_sem.at[turn]).wait()
        return jnp.maximum(jnp.max(mrecv[turn], axis=0), msend[turn])

    for dy in (-1, 1):
        side = (dy + 1) // 2
        for dx in (-1, 1):
            corner = (1 - dx) // 2 * 2 + 1 - side
            plane = 0 if dx == -1 else cx - 1
            send(ysend.at[side, plane], rxy.at[corner], dx, dy, 0)
            send(y1send.at[side], rxy1.at[corner], dx, dy, 0)
        send(ysend.at[side], ry.at[1 - side], 0, dy, 0)
    for dz in (-1, 1):
        side = (dz + 1) // 2
        for dx in (-1, 0, 1):
            for dy in (-1, 0, 1):
                send(zsend.at[side], rz.at[1 - dx, 1 - dy, 1 - side], dx, dy, dz)
    share(0)

    for copy in copies:
        copy.wait()

    in_body = lane < cz
    in_high = lane < cz + GHOST

    def ghosted(tile, high, low, c, x):
        slot = c * cx + x
        block, at = slot // slots, slot % slots * GHOST
        up = pltpu.roll(high[block], (cz - at) % LANES, 1)
        down = pltpu.roll(low[block], (LANES - GHOST - at) % LANES, 1)
        return jnp.where(in_body, tile, jnp.where(in_high, up, down))

    blocks = range(zsend.shape[1])
    for dx in range(3):
        plain = [[rz[dx, 1, side, block] for block in blocks] for side in (1, 0)]
        mixed = [[jnp.where(upper_half, rz[dx, 2, side, block], rz[dx, 0, side, block]) for block in blocks]
                 for side in (1, 0)]
        for x in range(cx):
            at = dx * cx + x
            near = dx == 1 or (dx == 0 and x == cx - 1) or (dx == 2 and x == 0)
            side_tiles = []
            if near:
                for pair in range(COMPS // 2):
                    if dx == 1:
                        below, above = ry[0, x, pair], ry[1, x, pair]
                    else:
                        below, above = rxy[dx // 2 * 2, pair], rxy[dx // 2 * 2 + 1, pair]
                    side_tiles.append(jnp.where(upper_half, above, below))
                    side_tiles.append(pltpu.roll(jnp.where(upper_half, below, above), GHOST, 0))
            else:
                below, above = rxy1[dx // 2 * 2, x], rxy1[dx // 2 * 2 + 1, x]
                for c in range(COMPS):
                    side_tiles.append(jnp.where(upper_half, pltpu.roll(above, (-c) % ROWS, 0),
                                                pltpu.roll(below, (ROWS - 1 - c) % ROWS, 0)))
            state_a, state_b = [], []
            for c in range(COMPS):
                tile = tiles[c][x] if dx == 1 else body(rx.at[dx // 2], c, x)
                state_a.append(ghosted(tile, plain[0], plain[1], c, x))
                state_b.append(ghosted(side_tiles[c], mixed[0], mixed[1], c, x))
            prim_a, prim_b = primitive_of(state_a), primitive_of(state_b)
            for c in range(COMPS):
                if dx == 1:
                    u[c, x] = state_a[c]
                q[c, at, 0:ROWS] = prim_a[c]
                q[c, at, ROWS:] = prim_b[c]

    now = gather(0)
    dt = courant / jnp.max(now, axis=1, keepdims=True)
    step = jnp.broadcast_to(dt, (2 * ROWS, LANES))
    half = 0.5 * step

    base = cx - 1
    count = cx + 2
    for i in range(count):
        at = base + i
        centre = [q[c, at] for c in range(COMPS)]
        for axis in range(3):
            edges = []
            for c in range(COMPS):
                if axis == 0:
                    near = [q[c, at + offset] for offset in (-3, -2, -1, 0, 1, 2, 3)]
                    lower = edge_of(*near[:6])
                    upper = edge_of(*near[1:])
                else:
                    near = [rolled(centre[c], offset, axis - 1) if offset else centre[c]
                            for offset in (-3, -2, -1, 0, 1, 2)]
                    lower = edge_of(*near)
                    upper = rolled(lower, 1, axis - 1)
                edges.append(limited(lower, upper, centre[c]))
            lower_faces, upper_faces = traced(centre, edges, axis, half)
            for c in range(COMPS):
                face[axis, 0, c, i] = lower_faces[c]
                face[axis, 1, c, i] = upper_faces[c]

    for i in range(count):
        for axis in range(3):
            if axis == 0 and i == 0:
                continue
            right = [face[axis, 0, c, i] for c in range(COMPS)]
            if axis == 0:
                left = [face[0, 1, c, i - 1] for c in range(COMPS)]
            else:
                left = [rolled(face[axis, 1, c, i], -1, axis - 1) for c in range(COMPS)]
            flux = hllc(left, right, axis)
            for c in range(COMPS):
                pred[axis, c, i] = flux[c] * half

    def differ(axis, c, i, rows):
        if axis == 0:
            return pred[0, c, i + 1, 0:rows] - pred[0, c, i, 0:rows]
        flux = pred[axis, c, i]
        return (rolled(flux, 1, axis - 1) - flux)[0:rows]

    def corrected(axis, i, rows):
        others = [other for other in range(3) if other != axis]
        change = [differ(others[0], c, i, rows) + differ(others[1], c, i, rows) for c in range(COMPS)]
        result = []
        for side in range(2):
            state = conserved_of([face[axis, side, c, i, 0:rows] for c in range(COMPS)])
            result.append(primitive_of([state[c] - change[c] for c in range(COMPS)]))
        return result

    total = [[u[c, x] for c in range(COMPS)] for x in range(cx)]
    thin = step[0:ROWS]
    before = corrected(0, 0, ROWS)
    flux_before = None
    for i in range(1, count):
        after = corrected(0, i, ROWS)
        flux = hllc(before[1], after[0], 0)
        if flux_before is not None:
            x = i - 2
            total[x] = [total[x][c] - thin * (flux[c] - flux_before[c]) for c in range(COMPS)]
        before, flux_before = after, flux
    best = None
    for x in range(cx):
        lower, upper = corrected(1, x + 1, 2 * ROWS)
        flux = hllc([rolled(item, -1, 0) for item in upper], lower, 1)
        total[x] = [total[x][c] - thin * (rolled(flux[c], 1, 0) - flux[c])[0:ROWS] for c in range(COMPS)]
        lower, upper = corrected(2, x + 1, ROWS)
        flux = hllc([rolled(item, -1, 1) for item in upper], lower, 2)
        total[x] = [total[x][c] - thin * (rolled(flux[c], 1, 1) - flux[c]) for c in range(COMPS)]
        for c in range(COMPS):
            out_ref[c, x] = total[x][c][:, 0:cz]
        speeds = signal_of(total[x])
        best = speeds if best is None else jnp.maximum(best, speeds)
    msend[1] = jnp.max(jnp.where(in_body, best, 0.0), axis=0, keepdims=True)
    share(1)
    next_ref[0, 0] = courant / jnp.max(gather(1))


def body(sizes, conserved_state):
    comps, cx, cy, cz = conserved_state.shape
    assert comps == COMPS and cx == GHOST and cy == ROWS and cz + 2 * GHOST <= LANES
    devices = sizes[0] * sizes[1] * sizes[2]
    blocks = -(-COMPS * cx * GHOST // LANES)
    f32 = jnp.float32
    vmem = lambda *shape: pltpu.VMEM(shape, f32)
    pairs = COMPS // 2
    messages = 2 + 8 + 2 + 18
    updated, following = pl.pallas_call(
        functools.partial(kernel, sizes),
        out_shape=(jax.ShapeDtypeStruct(conserved_state.shape, f32), jax.ShapeDtypeStruct((1, 1), f32)),
        in_specs=[pl.BlockSpec(memory_space=pl.ANY)],
        out_specs=(pl.BlockSpec(memory_space=pltpu.VMEM), pl.BlockSpec(memory_space=pltpu.SMEM)),
        scratch_shapes=[
            vmem(COMPS, cx, cy, cz),
            vmem(2, COMPS, cx, cy, cz),
            vmem(2, cx, pairs, ROWS, LANES),
            vmem(2, cx, pairs, ROWS, LANES),
            vmem(2, cx, ROWS, LANES),
            vmem(2, blocks, ROWS, LANES),
            vmem(3, 3, 2, blocks, ROWS, LANES),
            vmem(4, pairs, ROWS, LANES),
            vmem(4, cx, ROWS, LANES),
            vmem(COMPS, cx, ROWS, LANES),
            vmem(COMPS, 3 * cx, 2 * ROWS, LANES),
            vmem(3, 2, COMPS, cx + 2, 2 * ROWS, LANES),
            vmem(3, COMPS, cx + 2, 2 * ROWS, LANES),
            vmem(2, 1, LANES),
            vmem(2, devices - 1, 1, LANES),
            pltpu.SemaphoreType.DMA,
            pltpu.SemaphoreType.DMA((messages,)),
            pltpu.SemaphoreType.DMA((messages,)),
            pltpu.SemaphoreType.DMA((2,)),
            pltpu.SemaphoreType.DMA((2,)),
        ],
        compiler_params=pltpu.CompilerParams(collective_id=0, has_side_effects=True),
    )(conserved_state)
    return updated, following.reshape(())


def solution(mesh):
    sizes = tuple(mesh.shape[axis] for axis in ("gx", "gy", "gz"))
    return jax.shard_map(
        functools.partial(body, sizes),
        mesh=mesh,
        in_specs=(P(None, "gx", "gy", "gz"),),
        out_specs=(P(None, "gx", "gy", "gz"), P()),
        check_vma=False,
    )
```

```python
import functools

import jax
import jax.numpy as jnp
from jax import lax
from jax.experimental import pallas as pl
from jax.experimental.pallas import tpu as pltpu
from jax.sharding import PartitionSpec as P

GHOST = 4
ROWS = 8
UNROLL = 64
LANES = 128
COMPS = 6

adiabatic = 5.0 / 3.0
courant = 0.3
MESH_ID = pl.DeviceIdType.MESH


def primitive_of(u):
    inverse = 1.0 / u[0]
    velocity = [u[component] * inverse for component in (1, 2, 3)]
    kinetic = 0.5 * (u[1] * velocity[0] + u[2] * velocity[1] + u[3] * velocity[2])
    pressure = (adiabatic - 1.0) * (u[4] - kinetic)
    return [u[0], velocity[0], velocity[1], velocity[2], pressure, u[5] * inverse]


def conserved_of(q):
    density = q[0]
    momenta = [density * q[component] for component in (1, 2, 3)]
    kinetic = 0.5 * (momenta[0] * q[1] + momenta[1] * q[2] + momenta[2] * q[3])
    energy = q[4] * (1.0 / (adiabatic - 1.0)) + kinetic
    return [density, momenta[0], momenta[1], momenta[2], energy, density * q[5]]


def signal_of(u):
    q = primitive_of(u)
    sound = jnp.sqrt(adiabatic * q[4] / q[0])
    return jnp.maximum(jnp.maximum(jnp.abs(q[1]), jnp.abs(q[2])), jnp.abs(q[3])) + sound


def edge_of(b3, b2, b1, c, a1, a2):
    edge = (37.0 * (b1 + c) - 8.0 * (b2 + a1) + (b3 + a2)) * (1.0 / 60.0)
    return jnp.minimum(jnp.maximum(edge, jnp.minimum(b1, c)), jnp.maximum(b1, c))


def limited(lower, upper, centre):
    flatten = (upper - centre) * (centre - lower) <= 0.0
    spread = upper - lower
    skewed = spread * (centre - 0.5 * (lower + upper))
    limit = spread * spread * (1.0 / 6.0)
    new_lower = jnp.where(skewed > limit, 3.0 * centre - 2.0 * upper, lower)
    new_upper = jnp.where(skewed < -limit, 3.0 * centre - 2.0 * lower, upper)
    return jnp.where(flatten, centre, new_lower), jnp.where(flatten, centre, new_upper)


def traced(q, edges, axis, half):
    normal = 1 + axis
    slopes = [pair[1] - pair[0] for pair in edges]
    n = q[normal] * half
    rates = []
    for component in range(COMPS):
        rate = n * slopes[component]
        if component == 0:
            rate = rate + (q[0] * half) * slopes[normal]
        elif component == normal:
            rate = rate + (half / q[0]) * slopes[4]
        elif component == 4:
            rate = rate + (adiabatic * half) * q[4] * slopes[normal]
        rates.append(rate)
    lower = [edges[component][0] - rates[component] for component in range(COMPS)]
    upper = [edges[component][1] - rates[component] for component in range(COMPS)]
    return lower, upper


def hllc(left, right, axis):
    normal = 1 + axis
    t1, t2 = [component for component in (1, 2, 3) if component != normal]
    ratio_l = left[4] / left[0]
    ratio_r = right[4] / right[0]
    sound_l = jnp.sqrt(adiabatic * ratio_l)
    sound_r = jnp.sqrt(adiabatic * ratio_r)
    n_l, n_r = left[normal], right[normal]
    low = jnp.minimum(n_l - sound_l, n_r - sound_r)
    high = jnp.maximum(n_l + sound_l, n_r + sound_r)
    mass_l = left[0] * (low - n_l)
    mass_r = right[0] * (high - n_r)
    middle = (right[4] - left[4] + mass_l * n_l - mass_r * n_r) / (mass_l - mass_r)
    on_left = middle >= 0.0
    pick = lambda a, b: jnp.where(on_left, a, b)
    r, n, p = pick(left[0], right[0]), pick(n_l, n_r), pick(left[4], right[4])
    v, w, tracer = pick(left[t1], right[t1]), pick(left[t2], right[t2]), pick(left[5], right[5])
    ratio, mass = pick(ratio_l, ratio_r), pick(mass_l, mass_r)
    outer = pick(low, high)
    speed = pick(jnp.minimum(low, 0.0), jnp.maximum(high, 0.0))
    factor = mass / (outer - middle)
    flux = r * n + speed * (factor - r)
    gain = speed * factor * (middle - n)
    energy = ratio * (1.0 / (adiabatic - 1.0)) + 0.5 * (n * n + v * v + w * w)
    result = [None] * COMPS
    result[0] = flux
    result[normal] = n * flux + p + gain
    result[t1] = v * flux
    result[t2] = w * flux
    result[4] = energy * flux + n * p + gain * (middle + p / mass)
    result[5] = tracer * flux
    return result


def rolled(x, offset, axis):
    return pltpu.roll(x, (-offset) % x.shape[axis], axis)


def kernel(sizes, u_hbm, out_ref, next_ref, own, rx, ysend, ry, y1send, zsend, rz, rxy, rxy1, u, q,
           face, pred, msend, mrecv, own_sem, send_sem, recv_sem, msend_sem, mrecv_sem):
    nx, ny, nz = sizes
    devices = nx * ny * nz
    comps, cx, cy, cz = own.shape
    slots = LANES // GHOST
    ix, iy, iz = lax.axis_index("gx"), lax.axis_index("gy"), lax.axis_index("gz")
    me = (ix * ny + iy) * nz + iz

    load = pltpu.make_async_copy(u_hbm, own, own_sem)
    load.start()

    def place(k):
        target = lax.rem(me + k, devices)
        return (lax.div(target, ny * nz), lax.rem(lax.div(target, nz), ny), lax.rem(target, nz))

    barrier = pltpu.get_barrier_semaphore()

    def wrap(value, size):
        return jnp.where(value >= size, value - size, value)

    coordinates = [[wrap(index + k, size) for k in range(size)] if devices <= UNROLL else None
                   for index, size in ((ix, nx), (iy, ny), (iz, nz))]

    def everyone(act):
        if devices > UNROLL:
            def one(k, carry):
                act(k - 1, place(k))
                return carry
            lax.fori_loop(1, devices, one, 0)
            return
        far = [(min(kx, nx - kx) + min(ky, ny - ky) + min(kz, nz - kz), kx, ky, kz)
               for kx in range(nx) for ky in range(ny) for kz in range(nz)]
        for _, kx, ky, kz in sorted(far, reverse=True)[:-1]:
            act((kx * ny + ky) * nz + kz - 1, (coordinates[0][kx], coordinates[1][ky], coordinates[2][kz]))

    everyone(lambda slot, device: pl.semaphore_signal(barrier, inc=1, device_id=device, device_id_type=MESH_ID))
    load.wait()

    lane = lax.broadcasted_iota(jnp.int32, (ROWS, LANES), 1)
    row = lax.broadcasted_iota(jnp.int32, (ROWS, LANES), 0)
    upper_half = row < GHOST
    zero_tail = jnp.zeros((ROWS, LANES - cz), jnp.float32)

    def body(ref, c, x):
        return jnp.concatenate([ref[c, x], zero_tail], axis=1)

    tiles = [[body(own, c, x) for x in range(cx)] for c in range(COMPS)]
    best = None
    for x in range(cx):
        speeds = signal_of([tiles[c][x] for c in range(COMPS)])
        best = speeds if best is None else jnp.maximum(best, speeds)
    best = jnp.max(jnp.where(lane < cz, best, 0.0), axis=0, keepdims=True)
    msend[0] = best
    packs = [[None, None] for _ in range(zsend.shape[1])]
    for c in range(COMPS):
        for x in range(cx):
            slot = c * cx + x
            block, at = slot // slots, slot % slots * GHOST
            inside = (lane >= at) & (lane < at + GHOST)
            for side in range(2):
                start = 0 if side == 0 else cz - GHOST
                moved = pltpu.roll(tiles[c][x], (at - start) % LANES, 1)
                held = packs[block][side]
                packs[block][side] = moved if held is None else jnp.where(inside, moved, held)
    for block in range(zsend.shape[1]):
        for side in range(2):
            zsend[side, block] = packs[block][side]
    for x in range(cx):
        for pair in range(COMPS // 2):
            first, second = tiles[2 * pair][x], tiles[2 * pair + 1][x]
            swapped = pltpu.roll(second, GHOST, 0)
            ysend[0, x, pair] = jnp.where(upper_half, first, swapped)
            ysend[1, x, pair] = jnp.where(upper_half, swapped, first)
        for c in range(COMPS):
            y1send[0, x, c : c + 1] = tiles[c][x][0:1]
            y1send[1, x, c : c + 1] = tiles[c][x][ROWS - 1 : ROWS]

    pl.semaphore_wait(barrier, devices - 1)

    copies = []
    early, late = [], []

    def send(src, dst, dx, dy, dz):
        number = len(copies)
        copy = pltpu.make_async_remote_copy(
            src_ref=src, dst_ref=dst, send_sem=send_sem.at[number], recv_sem=recv_sem.at[number],
            device_id=(lax.rem(ix + dx + nx, nx), lax.rem(iy + dy + ny, ny), lax.rem(iz + dz + nz, nz)),
            device_id_type=MESH_ID)
        copy.start()
        copies.append(copy)
        if dx:
            late.append(copy)
        else:
            early.append(copy)

    for dx in (-1, 1):
        send(own, rx.at[(1 - dx) // 2], dx, 0, 0)

    def share(turn):
        everyone(lambda slot, device: pltpu.make_async_remote_copy(
            src_ref=msend.at[turn], dst_ref=mrecv.at[turn, slot], send_sem=msend_sem.at[turn],
            recv_sem=mrecv_sem.at[turn], device_id=device, device_id_type=MESH_ID).start())

    def gather(turn):
        pltpu.make_async_copy(mrecv.at[turn], mrecv.at[turn], mrecv_sem.at[turn]).wait()
        pltpu.make_async_copy(mrecv.at[turn], mrecv.at[turn], msend_sem.at[turn]).wait()
        return jnp.maximum(jnp.max(mrecv[turn], axis=0), msend[turn])

    for dy in (-1, 1):
        side = (dy + 1) // 2
        for dx in (-1, 1):
            corner = (1 - dx) // 2 * 2 + 1 - side
            plane = 0 if dx == -1 else cx - 1
            send(ysend.at[side, plane], rxy.at[corner], dx, dy, 0)
            send(y1send.at[side], rxy1.at[corner], dx, dy, 0)
        send(ysend.at[side], ry.at[1 - side], 0, dy, 0)
    for dz in (-1, 1):
        side = (dz + 1) // 2
        for dx in (-1, 0, 1):
            for dy in (-1, 0, 1):
                send(zsend.at[side], rz.at[1 - dx, 1 - dy, 1 - side], dx, dy, dz)
    share(0)

    for copy in early:
        copy.wait_recv()

    in_body = lane < cz
    in_high = lane < cz + GHOST

    def ghosted(tile, high, low, c, x):
        slot = c * cx + x
        block, at = slot // slots, slot % slots * GHOST
        up = pltpu.roll(high[block], (cz - at) % LANES, 1)
        down = pltpu.roll(low[block], (LANES - GHOST - at) % LANES, 1)
        return jnp.where(in_body, tile, jnp.where(in_high, up, down))

    blocks = range(zsend.shape[1])
    def assemble(dx):
        plain = [[rz[dx, 1, side, block] for block in blocks] for side in (1, 0)]
        mixed = [[jnp.where(upper_half, rz[dx, 2, side, block], rz[dx, 0, side, block]) for block in blocks]
                 for side in (1, 0)]
        for x in range(cx):
            at = dx * cx + x
            near = dx == 1 or (dx == 0 and x == cx - 1) or (dx == 2 and x == 0)
            side_tiles = []
            if near:
                for pair in range(COMPS // 2):
                    if dx == 1:
                        below, above = ry[0, x, pair], ry[1, x, pair]
                    else:
                        below, above = rxy[dx // 2 * 2, pair], rxy[dx // 2 * 2 + 1, pair]
                    side_tiles.append(jnp.where(upper_half, above, below))
                    side_tiles.append(pltpu.roll(jnp.where(upper_half, below, above), GHOST, 0))
            else:
                below, above = rxy1[dx // 2 * 2, x], rxy1[dx // 2 * 2 + 1, x]
                for c in range(COMPS):
                    side_tiles.append(jnp.where(upper_half, pltpu.roll(above, (-c) % ROWS, 0),
                                                pltpu.roll(below, (ROWS - 1 - c) % ROWS, 0)))
            state_a, state_b = [], []
            for c in range(COMPS):
                tile = tiles[c][x] if dx == 1 else body(rx.at[dx // 2], c, x)
                state_a.append(ghosted(tile, plain[0], plain[1], c, x))
                state_b.append(ghosted(side_tiles[c], mixed[0], mixed[1], c, x))
            prim_a, prim_b = primitive_of(state_a), primitive_of(state_b)
            for c in range(COMPS):
                if dx == 1:
                    u[c, x] = state_a[c]
                q[c, at, 0:ROWS] = prim_a[c]
                q[c, at, ROWS:] = prim_b[c]

    def trace(axis, i):
        at = base + i
        centre = [q[c, at] for c in range(COMPS)]
        edges = []
        for c in range(COMPS):
            if axis == 0:
                near = [q[c, at + offset] for offset in (-3, -2, -1, 0, 1, 2, 3)]
                lower = edge_of(*near[:6])
                upper = edge_of(*near[1:])
            else:
                near = [rolled(centre[c], offset, axis - 1) if offset else centre[c]
                        for offset in (-3, -2, -1, 0, 1, 2)]
                lower = edge_of(*near)
                upper = rolled(lower, 1, axis - 1)
            edges.append(limited(lower, upper, centre[c]))
        lower_faces, upper_faces = traced(centre, edges, axis, half)
        for c in range(COMPS):
            face[axis, 0, c, i] = lower_faces[c]
            face[axis, 1, c, i] = upper_faces[c]
        if axis:
            predict(axis, i, [rolled(item, -1, axis - 1) for item in upper_faces], lower_faces)
        elif i:
            predict(axis, i, [face[0, 1, c, i - 1] for c in range(COMPS)], lower_faces)

    def predict(axis, i, left, right):
        flux = hllc(left, right, axis)
        for c in range(COMPS):
            pred[axis, c, i] = flux[c] * half

    assemble(1)
    now = gather(0)
    dt = courant / jnp.max(now, axis=1, keepdims=True)
    step = jnp.broadcast_to(dt, (2 * ROWS, LANES))
    half = 0.5 * step

    base = cx - 1
    count = cx + 2
    for i in range(1, count - 1):
        for axis in (1, 2):
            trace(axis, i)
    for copy in late:
        copy.wait_recv()
    assemble(0)
    assemble(2)
    for i in range(count):
        trace(0, i)
        if i == 0 or i == count - 1:
            trace(1, i)
            trace(2, i)

    def differ(axis, c, i, rows):
        if axis == 0:
            return pred[0, c, i + 1, 0:rows] - pred[0, c, i, 0:rows]
        flux = pred[axis, c, i]
        return (rolled(flux, 1, axis - 1) - flux)[0:rows]

    def corrected(axis, i, rows):
        others = [other for other in range(3) if other != axis]
        change = [differ(others[0], c, i, rows) + differ(others[1], c, i, rows) for c in range(COMPS)]
        result = []
        for side in range(2):
            state = conserved_of([face[axis, side, c, i, 0:rows] for c in range(COMPS)])
            result.append(primitive_of([state[c] - change[c] for c in range(COMPS)]))
        return result

    total = [[u[c, x] for c in range(COMPS)] for x in range(cx)]
    thin = step[0:ROWS]
    before = corrected(0, 0, ROWS)
    flux_before = None
    for i in range(1, count):
        after = corrected(0, i, ROWS)
        flux = hllc(before[1], after[0], 0)
        if flux_before is not None:
            x = i - 2
            total[x] = [total[x][c] - thin * (flux[c] - flux_before[c]) for c in range(COMPS)]
        before, flux_before = after, flux
    best = None
    for x in range(cx):
        lower, upper = corrected(1, x + 1, 2 * ROWS)
        flux = hllc([rolled(item, -1, 0) for item in upper], lower, 1)
        total[x] = [total[x][c] - thin * (rolled(flux[c], 1, 0) - flux[c])[0:ROWS] for c in range(COMPS)]
        lower, upper = corrected(2, x + 1, ROWS)
        flux = hllc([rolled(item, -1, 1) for item in upper], lower, 2)
        total[x] = [total[x][c] - thin * (rolled(flux[c], 1, 1) - flux[c]) for c in range(COMPS)]
        for c in range(COMPS):
            out_ref[c, x] = total[x][c][:, 0:cz]
        speeds = signal_of(total[x])
        best = speeds if best is None else jnp.maximum(best, speeds)
    msend[1] = jnp.max(jnp.where(in_body, best, 0.0), axis=0, keepdims=True)
    share(1)
    for copy in copies:
        copy.wait_send()
    next_ref[0, 0] = courant / jnp.max(gather(1))


def body(sizes, conserved_state):
    comps, cx, cy, cz = conserved_state.shape
    assert comps == COMPS and cx == GHOST and cy == ROWS and cz + 2 * GHOST <= LANES
    devices = sizes[0] * sizes[1] * sizes[2]
    blocks = -(-COMPS * cx * GHOST // LANES)
    f32 = jnp.float32
    vmem = lambda *shape: pltpu.VMEM(shape, f32)
    pairs = COMPS // 2
    messages = 2 + 8 + 2 + 18
    updated, following = pl.pallas_call(
        functools.partial(kernel, sizes),
        out_shape=(jax.ShapeDtypeStruct(conserved_state.shape, f32), jax.ShapeDtypeStruct((1, 1), f32)),
        in_specs=[pl.BlockSpec(memory_space=pl.ANY)],
        out_specs=(pl.BlockSpec(memory_space=pltpu.VMEM), pl.BlockSpec(memory_space=pltpu.SMEM)),
        scratch_shapes=[
            vmem(COMPS, cx, cy, cz),
            vmem(2, COMPS, cx, cy, cz),
            vmem(2, cx, pairs, ROWS, LANES),
            vmem(2, cx, pairs, ROWS, LANES),
            vmem(2, cx, ROWS, LANES),
            vmem(2, blocks, ROWS, LANES),
            vmem(3, 3, 2, blocks, ROWS, LANES),
            vmem(4, pairs, ROWS, LANES),
            vmem(4, cx, ROWS, LANES),
            vmem(COMPS, cx, ROWS, LANES),
            vmem(COMPS, 3 * cx, 2 * ROWS, LANES),
            vmem(3, 2, COMPS, cx + 2, 2 * ROWS, LANES),
            vmem(3, COMPS, cx + 2, 2 * ROWS, LANES),
            vmem(2, 1, LANES),
            vmem(2, devices - 1, 1, LANES),
            pltpu.SemaphoreType.DMA,
            pltpu.SemaphoreType.DMA((messages,)),
            pltpu.SemaphoreType.DMA((messages,)),
            pltpu.SemaphoreType.DMA((2,)),
            pltpu.SemaphoreType.DMA((2,)),
        ],
        compiler_params=pltpu.CompilerParams(collective_id=0, has_side_effects=True),
    )(conserved_state)
    return updated, following.reshape(())


def solution(mesh):
    sizes = tuple(mesh.shape[axis] for axis in ("gx", "gy", "gz"))
    return jax.shard_map(
        functools.partial(body, sizes),
        mesh=mesh,
        in_specs=(P(None, "gx", "gy", "gz"),),
        out_specs=(P(None, "gx", "gy", "gz"), P()),
        check_vma=False,
    )
```

```python
import functools

import jax
import jax.numpy as jnp
from jax import lax
from jax.experimental import pallas as pl
from jax.experimental.pallas import tpu as pltpu
from jax.sharding import PartitionSpec as P

GHOST = 4
ROWS = 8
LANES = 128
COMPS = 6

adiabatic = 5.0 / 3.0
courant = 0.3
MESH_ID = pl.DeviceIdType.MESH


def primitive_of(u):
    inverse = 1.0 / u[0]
    velocity = [u[component] * inverse for component in (1, 2, 3)]
    kinetic = 0.5 * (u[1] * velocity[0] + u[2] * velocity[1] + u[3] * velocity[2])
    pressure = (adiabatic - 1.0) * (u[4] - kinetic)
    return [u[0], velocity[0], velocity[1], velocity[2], pressure, u[5] * inverse]


def conserved_of(q):
    density = q[0]
    momenta = [density * q[component] for component in (1, 2, 3)]
    kinetic = 0.5 * (momenta[0] * q[1] + momenta[1] * q[2] + momenta[2] * q[3])
    energy = q[4] * (1.0 / (adiabatic - 1.0)) + kinetic
    return [density, momenta[0], momenta[1], momenta[2], energy, density * q[5]]


def signal_of(u):
    q = primitive_of(u)
    sound = jnp.sqrt(adiabatic * q[4] / q[0])
    return jnp.maximum(jnp.maximum(jnp.abs(q[1]), jnp.abs(q[2])), jnp.abs(q[3])) + sound


def edge_of(b3, b2, b1, c, a1, a2):
    edge = (37.0 * (b1 + c) - 8.0 * (b2 + a1) + (b3 + a2)) * (1.0 / 60.0)
    return jnp.minimum(jnp.maximum(edge, jnp.minimum(b1, c)), jnp.maximum(b1, c))


def limited(lower, upper, centre):
    flatten = (upper - centre) * (centre - lower) <= 0.0
    spread = upper - lower
    skewed = spread * (centre - 0.5 * (lower + upper))
    limit = spread * spread * (1.0 / 6.0)
    new_lower = jnp.where(skewed > limit, 3.0 * centre - 2.0 * upper, lower)
    new_upper = jnp.where(skewed < -limit, 3.0 * centre - 2.0 * lower, upper)
    return jnp.where(flatten, centre, new_lower), jnp.where(flatten, centre, new_upper)


def traced(q, edges, axis, half):
    normal = 1 + axis
    slopes = [pair[1] - pair[0] for pair in edges]
    n = q[normal] * half
    rates = []
    for component in range(COMPS):
        rate = n * slopes[component]
        if component == 0:
            rate = rate + (q[0] * half) * slopes[normal]
        elif component == normal:
            rate = rate + (half / q[0]) * slopes[4]
        elif component == 4:
            rate = rate + (adiabatic * half) * q[4] * slopes[normal]
        rates.append(rate)
    lower = [edges[component][0] - rates[component] for component in range(COMPS)]
    upper = [edges[component][1] - rates[component] for component in range(COMPS)]
    return lower, upper


def hllc(left, right, axis):
    normal = 1 + axis
    t1, t2 = [component for component in (1, 2, 3) if component != normal]
    ratio_l = left[4] / left[0]
    ratio_r = right[4] / right[0]
    sound_l = jnp.sqrt(adiabatic * ratio_l)
    sound_r = jnp.sqrt(adiabatic * ratio_r)
    n_l, n_r = left[normal], right[normal]
    low = jnp.minimum(n_l - sound_l, n_r - sound_r)
    high = jnp.maximum(n_l + sound_l, n_r + sound_r)
    mass_l = left[0] * (low - n_l)
    mass_r = right[0] * (high - n_r)
    middle = (right[4] - left[4] + mass_l * n_l - mass_r * n_r) / (mass_l - mass_r)
    on_left = middle >= 0.0
    pick = lambda a, b: jnp.where(on_left, a, b)
    r, n, p = pick(left[0], right[0]), pick(n_l, n_r), pick(left[4], right[4])
    v, w, tracer = pick(left[t1], right[t1]), pick(left[t2], right[t2]), pick(left[5], right[5])
    ratio, mass = pick(ratio_l, ratio_r), pick(mass_l, mass_r)
    outer = pick(low, high)
    speed = pick(jnp.minimum(low, 0.0), jnp.maximum(high, 0.0))
    factor = mass / (outer - middle)
    flux = r * n + speed * (factor - r)
    gain = speed * factor * (middle - n)
    energy = ratio * (1.0 / (adiabatic - 1.0)) + 0.5 * (n * n + v * v + w * w)
    result = [None] * COMPS
    result[0] = flux
    result[normal] = n * flux + p + gain
    result[t1] = v * flux
    result[t2] = w * flux
    result[4] = energy * flux + n * p + gain * (middle + p / mass)
    result[5] = tracer * flux
    return result


def rolled(x, offset, axis):
    return pltpu.roll(x, (-offset) % x.shape[axis], axis)


def kernel(sizes, u_hbm, out_ref, next_ref, own, rx, ysend, ry, corner_send, zsend, rz, rxy, u, q,
           face, pred, msend, mrecv_x, mrecv_yz, own_sem, send_sem, recv_sem, msend_sem, mrecv_sem):
    nx, ny, nz = sizes
    comps, cx, cy, cz = own.shape
    slots = LANES // GHOST
    mrecv = (mrecv_x, mrecv_yz)
    ix, iy, iz = lax.axis_index("gx"), lax.axis_index("gy"), lax.axis_index("gz")
    load = pltpu.make_async_copy(u_hbm, own, own_sem)
    load.start()

    barrier = pltpu.get_barrier_semaphore()

    def wrap(value, size):
        return jnp.where(value >= size, value - size, value)

    coordinates = [[wrap(index + k, size) for k in range(size)] for index, size in ((ix, nx), (iy, ny), (iz, nz))]

    def device_at(offset):
        return tuple(coordinates[axis][offset[axis] % sizes[axis]] for axis in range(3))

    def hops(offset):
        return sum(min(k % size, -k % size) for k, size in zip(offset, sizes))

    groups = [[(k, 0, 0) for k in range(1, nx)],
              [(0, k // nz, k % nz) for k in range(1, ny * nz)]]
    around = [(dx % nx, dy % ny, dz % nz) for dx in (-1, 0, 1) for dy in (-1, 0, 1) for dz in (-1, 0, 1)]
    partners = sorted(set(around + groups[0] + groups[1]) - {(0, 0, 0)}, key=lambda o: (-hops(o), o))
    for offset in partners:
        pl.semaphore_signal(barrier, inc=1, device_id=device_at(offset), device_id_type=MESH_ID)
    load.wait()

    lane = lax.broadcasted_iota(jnp.int32, (ROWS, LANES), 1)
    row = lax.broadcasted_iota(jnp.int32, (ROWS, LANES), 0)
    upper_half = row < GHOST
    zero_tail = jnp.zeros((ROWS, LANES - cz), jnp.float32)

    def body(ref, c, x):
        return jnp.concatenate([ref[c, x], zero_tail], axis=1)

    tiles = [[body(own, c, x) for x in range(cx)] for c in range(COMPS)]
    best = None
    for x in range(cx):
        speeds = signal_of([tiles[c][x] for c in range(COMPS)])
        best = speeds if best is None else jnp.maximum(best, speeds)
    best = jnp.max(jnp.where(lane < cz, best, 0.0), axis=0, keepdims=True)
    msend[0, 0] = best
    packs = [[None, None] for _ in range(zsend.shape[1])]
    for c in range(COMPS):
        for x in range(cx):
            slot = c * cx + x
            block, at = slot // slots, slot % slots * GHOST
            inside = (lane >= at) & (lane < at + GHOST)
            for side in range(2):
                start = 0 if side == 0 else cz - GHOST
                moved = pltpu.roll(tiles[c][x], (at - start) % LANES, 1)
                held = packs[block][side]
                packs[block][side] = moved if held is None else jnp.where(inside, moved, held)
    for block in range(zsend.shape[1]):
        for side in range(2):
            zsend[side, block] = packs[block][side]
    for x in range(cx):
        for pair in range(COMPS // 2):
            first, second = tiles[2 * pair][x], tiles[2 * pair + 1][x]
            swapped = pltpu.roll(second, GHOST, 0)
            below, above = jnp.where(upper_half, first, swapped), jnp.where(upper_half, swapped, first)
            ysend[0, x, pair] = below
            ysend[1, x, pair] = above
            for side, plane in ((0, 0), (1, cx - 1)):
                if x == plane:
                    corner_send[0, side, pair] = below
                    corner_send[1, side, pair] = above

    for side, skipped in ((0, 0), (1, cx - 1)):
        for number, x in enumerate(x for x in range(cx) if x != skipped):
            for c in range(COMPS):
                corner_send[0, side, COMPS // 2 + number, c : c + 1] = tiles[c][x][0:1]
                corner_send[1, side, COMPS // 2 + number, c : c + 1] = tiles[c][x][ROWS - 1 : ROWS]

    pl.semaphore_wait(barrier, len(partners))

    copies = []
    early, late = [], []

    def send(src, dst, dx, dy, dz):
        number = len(copies)
        copy = pltpu.make_async_remote_copy(
            src_ref=src, dst_ref=dst, send_sem=send_sem.at[number], recv_sem=recv_sem.at[number],
            device_id=device_at((dx, dy, dz)), device_id_type=MESH_ID)
        copy.start()
        copies.append(copy)
        if dx:
            late.append(copy)
        else:
            early.append(copy)

    def share(turn, phase):
        for slot, offset in enumerate(groups[phase]):
            pltpu.make_async_remote_copy(
                src_ref=msend.at[turn, phase], dst_ref=mrecv[phase].at[turn, slot],
                send_sem=msend_sem.at[turn, phase], recv_sem=mrecv_sem.at[turn, phase],
                device_id=device_at(offset), device_id_type=MESH_ID).start()

    def gather(turn, phase):
        held = mrecv[phase].at[turn]
        pltpu.make_async_copy(held, held, mrecv_sem.at[turn, phase]).wait()
        return jnp.maximum(jnp.max(held[...], axis=0), msend[turn, phase])

    share(0, 0)
    for dx in (-1, 1):
        send(own, rx.at[(1 - dx) // 2], dx, 0, 0)
    for dy in (0, -1, 1):
        for dz in (-1, 1):
            side = (dz + 1) // 2
            send(zsend.at[side], rz.at[1, 1 - dy, 1 - side], 0, dy, dz)
        if dy:
            side = (dy + 1) // 2
            send(ysend.at[side], ry.at[1 - side], 0, dy, 0)
    for dx in (-1, 1):
        for dy in (-1, 1):
            side = (dy + 1) // 2
            send(corner_send.at[side, (dx + 1) // 2], rxy.at[(1 - dx) // 2 * 2 + 1 - side], dx, dy, 0)
        for dy in (-1, 0, 1):
            for dz in (-1, 1):
                side = (dz + 1) // 2
                send(zsend.at[side], rz.at[1 - dx, 1 - dy, 1 - side], dx, dy, dz)
    msend[0, 1] = gather(0, 0)
    share(0, 1)

    for copy in early:
        copy.wait_recv()

    in_body = lane < cz
    in_high = lane < cz + GHOST

    def ghosted(tile, high, low, c, x):
        slot = c * cx + x
        block, at = slot // slots, slot % slots * GHOST
        up = pltpu.roll(high[block], (cz - at) % LANES, 1)
        down = pltpu.roll(low[block], (LANES - GHOST - at) % LANES, 1)
        return jnp.where(in_body, tile, jnp.where(in_high, up, down))

    blocks = range(zsend.shape[1])
    def assemble(dx):
        plain = [[rz[dx, 1, side, block] for block in blocks] for side in (1, 0)]
        mixed = [[jnp.where(upper_half, rz[dx, 2, side, block], rz[dx, 0, side, block]) for block in blocks]
                 for side in (1, 0)]
        for x in range(cx):
            at = dx * cx + x
            near = dx == 1 or (dx == 0 and x == cx - 1) or (dx == 2 and x == 0)
            side_tiles = []
            if near:
                for pair in range(COMPS // 2):
                    if dx == 1:
                        below, above = ry[0, x, pair], ry[1, x, pair]
                    else:
                        below, above = rxy[dx // 2 * 2, pair], rxy[dx // 2 * 2 + 1, pair]
                    side_tiles.append(jnp.where(upper_half, above, below))
                    side_tiles.append(pltpu.roll(jnp.where(upper_half, below, above), GHOST, 0))
            else:
                number = COMPS // 2 + (x if dx == 0 else x - 1)
                below, above = rxy[dx // 2 * 2, number], rxy[dx // 2 * 2 + 1, number]
                for c in range(COMPS):
                    side_tiles.append(jnp.where(upper_half, pltpu.roll(above, (-c) % ROWS, 0),
                                                pltpu.roll(below, (ROWS - 1 - c) % ROWS, 0)))
            state_a, state_b = [], []
            for c in range(COMPS):
                tile = tiles[c][x] if dx == 1 else body(rx.at[dx // 2], c, x)
                state_a.append(ghosted(tile, plain[0], plain[1], c, x))
                state_b.append(ghosted(side_tiles[c], mixed[0], mixed[1], c, x))
            prim_a, prim_b = primitive_of(state_a), primitive_of(state_b)
            for c in range(COMPS):
                if dx == 1:
                    u[c, x] = state_a[c]
                q[c, at, 0:ROWS] = prim_a[c]
                q[c, at, ROWS:] = prim_b[c]

    def trace(axis, i):
        at = base + i
        centre = [q[c, at] for c in range(COMPS)]
        edges = []
        for c in range(COMPS):
            if axis == 0:
                near = [q[c, at + offset] for offset in (-3, -2, -1, 0, 1, 2, 3)]
                lower = edge_of(*near[:6])
                upper = edge_of(*near[1:])
            else:
                near = [rolled(centre[c], offset, axis - 1) if offset else centre[c]
                        for offset in (-3, -2, -1, 0, 1, 2)]
                lower = edge_of(*near)
                upper = rolled(lower, 1, axis - 1)
            edges.append(limited(lower, upper, centre[c]))
        lower_faces, upper_faces = traced(centre, edges, axis, half)
        for c in range(COMPS):
            face[axis, 0, c, i] = lower_faces[c]
            face[axis, 1, c, i] = upper_faces[c]
        if axis:
            predict(axis, i, [rolled(item, -1, axis - 1) for item in upper_faces], lower_faces)
        elif i:
            predict(axis, i, [face[0, 1, c, i - 1] for c in range(COMPS)], lower_faces)

    def predict(axis, i, left, right):
        flux = hllc(left, right, axis)
        for c in range(COMPS):
            pred[axis, c, i] = flux[c] * half

    assemble(1)
    now = gather(0, 1)
    dt = courant / jnp.max(now, axis=1, keepdims=True)
    step = jnp.broadcast_to(dt, (2 * ROWS, LANES))
    half = 0.5 * step

    base = cx - 1
    count = cx + 2
    for i in range(1, count - 1):
        for axis in (1, 2):
            trace(axis, i)
    for copy in late:
        copy.wait_recv()
    assemble(0)
    assemble(2)
    for i in range(count):
        trace(0, i)
        if i == 0 or i == count - 1:
            trace(1, i)
            trace(2, i)

    def differ(axis, c, i, rows):
        if axis == 0:
            return pred[0, c, i + 1, 0:rows] - pred[0, c, i, 0:rows]
        flux = pred[axis, c, i]
        return (rolled(flux, 1, axis - 1) - flux)[0:rows]

    def corrected(axis, i, rows):
        others = [other for other in range(3) if other != axis]
        change = [differ(others[0], c, i, rows) + differ(others[1], c, i, rows) for c in range(COMPS)]
        result = []
        for side in range(2):
            state = conserved_of([face[axis, side, c, i, 0:rows] for c in range(COMPS)])
            result.append(primitive_of([state[c] - change[c] for c in range(COMPS)]))
        return result

    total = [[u[c, x] for c in range(COMPS)] for x in range(cx)]
    thin = step[0:ROWS]
    before = corrected(0, 0, ROWS)
    flux_before = None
    for i in range(1, count):
        after = corrected(0, i, ROWS)
        flux = hllc(before[1], after[0], 0)
        if flux_before is not None:
            x = i - 2
            total[x] = [total[x][c] - thin * (flux[c] - flux_before[c]) for c in range(COMPS)]
        before, flux_before = after, flux
    best = None
    for x in range(cx):
        lower, upper = corrected(1, x + 1, 2 * ROWS)
        flux = hllc([rolled(item, -1, 0) for item in upper], lower, 1)
        total[x] = [total[x][c] - thin * (rolled(flux[c], 1, 0) - flux[c])[0:ROWS] for c in range(COMPS)]
        lower, upper = corrected(2, x + 1, ROWS)
        flux = hllc([rolled(item, -1, 1) for item in upper], lower, 2)
        total[x] = [total[x][c] - thin * (rolled(flux[c], 1, 1) - flux[c]) for c in range(COMPS)]
        for c in range(COMPS):
            out_ref[c, x] = total[x][c][:, 0:cz]
        speeds = signal_of(total[x])
        best = speeds if best is None else jnp.maximum(best, speeds)
    msend[1, 0] = jnp.max(jnp.where(in_body, best, 0.0), axis=0, keepdims=True)
    share(1, 0)
    for copy in copies:
        copy.wait_send()
    msend[1, 1] = gather(1, 0)
    share(1, 1)
    result = courant / jnp.max(gather(1, 1))
    for turn in range(2):
        for phase in range(2):
            held = mrecv[phase].at[turn]
            pltpu.make_async_copy(held, held, msend_sem.at[turn, phase]).wait()
    next_ref[0, 0] = result


def body(sizes, conserved_state):
    comps, cx, cy, cz = conserved_state.shape
    assert comps == COMPS and cx == GHOST and cy == ROWS and cz + 2 * GHOST <= LANES
    blocks = -(-COMPS * cx * GHOST // LANES)
    f32 = jnp.float32
    vmem = lambda *shape: pltpu.VMEM(shape, f32)
    pairs = COMPS // 2
    messages = 2 + 4 + 2 + 18
    updated, following = pl.pallas_call(
        functools.partial(kernel, sizes),
        out_shape=(jax.ShapeDtypeStruct(conserved_state.shape, f32), jax.ShapeDtypeStruct((1, 1), f32)),
        in_specs=[pl.BlockSpec(memory_space=pl.ANY)],
        out_specs=(pl.BlockSpec(memory_space=pltpu.VMEM), pl.BlockSpec(memory_space=pltpu.SMEM)),
        scratch_shapes=[
            vmem(COMPS, cx, cy, cz),
            vmem(2, COMPS, cx, cy, cz),
            vmem(2, cx, pairs, ROWS, LANES),
            vmem(2, cx, pairs, ROWS, LANES),
            vmem(2, 2, pairs + cx - 1, ROWS, LANES),
            vmem(2, blocks, ROWS, LANES),
            vmem(3, 3, 2, blocks, ROWS, LANES),
            vmem(4, pairs + cx - 1, ROWS, LANES),
            vmem(COMPS, cx, ROWS, LANES),
            vmem(COMPS, 3 * cx, 2 * ROWS, LANES),
            vmem(3, 2, COMPS, cx + 2, 2 * ROWS, LANES),
            vmem(3, COMPS, cx + 2, 2 * ROWS, LANES),
            vmem(2, 2, 1, LANES),
            vmem(2, sizes[0] - 1, 1, LANES),
            vmem(2, sizes[1] * sizes[2] - 1, 1, LANES),
            pltpu.SemaphoreType.DMA,
            pltpu.SemaphoreType.DMA((messages,)),
            pltpu.SemaphoreType.DMA((messages,)),
            pltpu.SemaphoreType.DMA((2, 2)),
            pltpu.SemaphoreType.DMA((2, 2)),
        ],
        compiler_params=pltpu.CompilerParams(collective_id=0, has_side_effects=True),
    )(conserved_state)
    return updated, following.reshape(())


def solution(mesh):
    sizes = tuple(mesh.shape[axis] for axis in ("gx", "gy", "gz"))
    return jax.shard_map(
        functools.partial(body, sizes),
        mesh=mesh,
        in_specs=(P(None, "gx", "gy", "gz"),),
        out_specs=(P(None, "gx", "gy", "gz"), P()),
        check_vma=False,
    )
```
